32 devices in a mesh: mem: 8 (over y, x, core), strip: 4 (over z).
Axes of the slice: x: 2, y: 2, z: 4, core: 2. Of those that a mesh axis runs over, the one named last changes fastest.
Arguments:
- state: float32 [128, 3, 32768], P('mem', None, 'strip'), may hold values from -6 to 6
- courant: float32 [32768], P('strip'), may hold values from 0.5 to 0.95
- angle: float32 [32768], P('strip'), may hold values from -0.4 to 0.4
- obs_index: int32 [2048], P('strip'), may hold values from 0 to 8191
- obs_value: float32 [2048], P('strip'), may hold values from -6 to 6
- obs_variance: float32 [2048], P('strip'), may hold values from 0.1 to 1
- perturb: float32 [128, 2048], P(None, 'strip'), may hold values from -4 to 4
Outputs:
- forecast: float32 [128, 3, 32768], P('mem', None, 'strip')
The draws below stay inside these ranges and needn't reach their ends.
All inputs are finite; a program needn't handle non-finite values.
Results may differ from the reference program's by a relative error of at most 0.00014.
Values sent between devices are 32-bit elements; how exact they have to be, the bound alone decides.
No kernel may reach another device: no remote copies, remote signals or barrier semaphores. Data moves between devices by JAX's collectives and lax.ppermute only.
A program may use at most 128 MiB of HBM per device.

```python
import math
import jax
import jax.numpy as jnp
from jax import lax

COLS_DEV = 8192
NOBS = 512
STEPS_BEFORE = 4
STEPS_AFTER = 2
MEMBERS = 128
COLUMNS = 32768
ALL_OBS = 2048


def set_ends(array, own_key, smallest, high):
    place = [jax.random.randint(jax.random.fold_in(own_key, axis), (), 0, length) for axis, length in enumerate(array.shape)]
    widest = array.shape.index(max(array.shape))
    neighbour = place[:widest] + [(place[widest] + 1) % array.shape[widest]] + place[widest + 1:]
    return array.at[tuple(place)].set(smallest).at[tuple(neighbour)].set(high)


def level_of(stream_key, dims, pieces, low, high):
    def one(axis_at, blocks):
        heights = jax.random.uniform(jax.random.fold_in(jax.random.fold_in(stream_key, 6), axis_at), (blocks,), jnp.float32, low / len(pieces), high / len(pieces))
        return jnp.repeat(jnp.exp(heights), dims[axis_at] // blocks).reshape((-1,) + (1,) * (len(dims) - axis_at - 1))

    level = one(*pieces[0])
    for cut in pieces[1:]:
        level = level * one(*cut)
    return level


def gaussian(own_key, shape, width, most, shards=(), kind=jnp.bfloat16):
    values = jax.random.normal(own_key, shape, jnp.float32) * width
    if len(shards) > 0:
        values = level_of(own_key, shape, shards, -0.22, 0.18) * values
    return jnp.clip(values, min=-most, max=most).astype(kind)


def setup_inputs(seed: int = 0) -> dict:
    seeds = jax.random.split(jax.random.key(seed), 8)
    return {
        "state": gaussian(seeds[0], (MEMBERS, 3, COLUMNS), 1.0, 6.0, ((0, 8), (2, 4)), jnp.float32),
        "courant": jnp.clip(0.5 + 0.45 * jax.random.uniform(seeds[1], (COLUMNS,), jnp.float32) ** level_of(seeds[1], (COLUMNS,), ((0, 4),), -0.2, 0.2), 0.5, 0.95),
        "angle": jnp.clip(jax.random.uniform(seeds[2], (COLUMNS,), jnp.float32, -0.4, 0.4) * level_of(seeds[2], (COLUMNS,), ((0, 4),), -0.4, 0.0), -0.4, 0.4),
        "obs_index": set_ends(jax.random.randint(seeds[3], (ALL_OBS,), 0, COLS_DEV), jax.random.fold_in(seeds[3], 1), 0, COLS_DEV - 1).astype(jnp.int32),
        "obs_value": gaussian(seeds[4], (ALL_OBS,), 1.0, 6.0, ((0, 4),), jnp.float32),
        "obs_variance": jnp.clip(jnp.exp(math.log(1.0) - 2.3025851 * jax.random.uniform(seeds[5], (ALL_OBS,), jnp.float32) ** level_of(seeds[5], (ALL_OBS,), ((0, 4),), -0.2, 0.2)), 0.1, 1.0),
        "perturb": gaussian(seeds[6], (MEMBERS, ALL_OBS), 0.5, 4.0, ((1, 4),), jnp.float32),
    }


HIGH = lax.Precision.HIGHEST

def advance(state, courant, angle):
    height = state[:, 0]
    speed = state[:, 1]
    across = state[:, 2]
    right_wave = speed + height
    left_wave = speed - height
    right_new = right_wave - courant * (right_wave - jnp.roll(right_wave, 1, axis=-1))
    left_new = left_wave + courant * (jnp.roll(left_wave, -1, axis=-1) - left_wave)
    speed_new = 0.5 * (right_new + left_new)
    height_new = 0.5 * (right_new - left_new)
    cosine = jnp.cos(angle)
    sine = jnp.sin(angle)
    speed_out = cosine * speed_new + sine * across
    across_out = cosine * across - sine * speed_new
    return jnp.stack([height_new, speed_out, across_out], axis=1)

def gain(predicted, obs_value, perturb, obs_variance):
    count = predicted.shape[0]
    spread = predicted - jnp.mean(predicted, axis=0)
    innovation = obs_value[None, :] + perturb - predicted
    cov = jnp.dot(spread.T, spread, precision=HIGH) / (count - 1) + jnp.diag(obs_variance)
    factor = jnp.linalg.cholesky(cov)
    solved = jax.scipy.linalg.cho_solve((factor, True), innovation.T)
    return jnp.dot(spread, solved, precision=HIGH) / (count - 1)

def reference(state, courant, angle, obs_index, obs_value, obs_variance, perturb):
    for step in range(STEPS_BEFORE):
        state = advance(state, courant, angle)
    count = state.shape[0]
    strips = COLUMNS // COLS_DEV
    offsets = jnp.arange(strips * NOBS, dtype=jnp.int32) // NOBS * COLS_DEV
    columns = obs_index.astype(jnp.int32) + offsets
    predicted = state[:, 0][:, columns]
    predicted = predicted.reshape(count, strips, NOBS).transpose(1, 0, 2)
    pert = perturb.reshape(count, strips, NOBS).transpose(1, 0, 2)
    weights = lax.map(lambda group: gain(*group), (predicted, obs_value.reshape(strips, NOBS), pert, obs_variance.reshape(strips, NOBS)))
    grid = state.reshape(count, 3, strips, COLS_DEV)
    grid = grid + jnp.einsum('skm,kfsc->mfsc', weights, grid, precision=HIGH)
    state = grid.reshape(count, 3, strips * COLS_DEV)
    for step in range(STEPS_AFTER):
        state = advance(state, courant, angle)
    return state
```

```python
import functools

import jax
import jax.numpy as jnp
from jax import lax
from jax.experimental import pallas as pl
from jax.experimental.pallas import tpu as pltpu
from jax.sharding import PartitionSpec as P

STEPS_BEFORE = 4
STEPS_AFTER = 2
LANES = 128
ROWS = 8

HIGH = lax.Precision.HIGHEST

VMEM = pl.BlockSpec(memory_space=pltpu.VMEM)
SMEM = pl.BlockSpec(memory_space=pltpu.SMEM)
ANY = pl.BlockSpec(memory_space=pl.ANY)


def shifted(block, axis, distance):
    count = lax.axis_size(axis)
    return lax.ppermute(block, axis, [(i, (i + distance) % count) for i in range(count)])


def product(left, right, contract):
    return lax.dot_general(left, right, (contract, ((), ())), precision=HIGH, preferred_element_type=jnp.float32)


def step(height, speed, across, courant, cosine, sine):
    width = height.shape[1]
    right_wave = speed + height
    left_wave = speed - height
    right_new = right_wave - courant * (right_wave - pltpu.roll(right_wave, 1, 1))
    left_new = left_wave + courant * (pltpu.roll(left_wave, width - 1, 1) - left_wave)
    speed_new = 0.5 * (right_new + left_new)
    height_new = 0.5 * (right_new - left_new)
    return height_new, cosine * speed_new + sine * across, cosine * across - sine * speed_new


def advance_kernel(me_ref, index_ref, state_ref, behind_ref, ahead_ref, coef_ref, out_ref, seen_ref,
                   wide_ref, coefs_ref, prior_ref, edge_ref, sems):
    fields, members, columns = state_ref.shape
    parts, block = out_ref.shape[0], out_ref.shape[3]
    copies = [
        pltpu.make_async_copy(state_ref.at[f], wide_ref.at[f, :, pl.ds(LANES, columns)], sems.at[f])
        for f in range(fields)
    ]
    for copy in copies:
        copy.start()
    for f in range(fields):
        wide_ref[f, :, :LANES] = behind_ref[f * members:(f + 1) * members, :]
        wide_ref[f, :, LANES + columns:] = ahead_ref[f * members:(f + 1) * members, :]
    coefs_ref[:, :LANES] = behind_ref[fields * members:, :]
    coefs_ref[:, LANES:LANES + columns] = coef_ref[...]
    coefs_ref[:, LANES + columns:] = ahead_ref[fields * members:, :]
    for copy in copies:
        copy.wait()
    me = me_ref[0]
    width = block + 2 * LANES
    groups = members // ROWS

    def one(turn, _):
        away = turn // groups
        rows = pl.ds(pl.multiple_of((turn % groups) * ROWS, ROWS), ROWS)
        part = lax.rem(me + away, parts)
        start = pl.multiple_of(part * block, LANES)
        lanes = pl.ds(start, width)
        fields_now = [wide_ref[f, rows, lanes] for f in range(fields)]
        coefs = [jnp.broadcast_to(coefs_ref[k:k + 1, lanes], (ROWS, width)) for k in range(3)]
        for _ in range(STEPS_BEFORE):
            fields_now = step(*fields_now, *coefs)
        column = lax.broadcasted_iota(jnp.int32, (ROWS, width), 1) + (start - LANES)
        inside = (column >= 0) & (column < columns)
        fields_now = [jnp.where(inside, value, 0.0) for value in fields_now]
        prior_ref[rows, pl.ds(start, block)] = fields_now[0][:, LANES:LANES + block]
        for _ in range(STEPS_AFTER):
            fields_now = step(*fields_now, *coefs)
        for f in range(fields):
            out_ref[away, f, rows, :] = fields_now[f][:, LANES:LANES + block]

        @pl.when(part == 0)
        def _():
            for f in range(fields):
                edge_ref[0, f, rows, :] = fields_now[f][:, :LANES]

        @pl.when(part == parts - 1)
        def _():
            for f in range(fields):
                edge_ref[1, f, rows, :] = fields_now[f][:, LANES + block:]
        return 0

    lax.fori_loop(0, parts * groups, one, 0)

    lane = lax.broadcasted_iota(jnp.int32, (members, LANES), 1)
    for group in range(index_ref.shape[0] // LANES):
        def pick(o, held):
            index = index_ref[group * LANES + o]
            tile = prior_ref[:, pl.ds(pl.multiple_of((index // LANES) * LANES, LANES), LANES)]
            turned = pltpu.roll(tile, (o - index % LANES + LANES) % LANES, 1)
            return jnp.where(lane == o, turned, held)
        held = lax.fori_loop(0, LANES, pick, jnp.zeros((members, LANES), jnp.float32), unroll=8)
        seen_ref[:, group * LANES:(group + 1) * LANES] = held
    packed = jnp.zeros((members, LANES), jnp.float32)
    for f in range(fields):
        for side in range(2):
            at = (side * fields + f) * STEPS_AFTER
            turn = at + (STEPS_AFTER if side == 0 else 0)
            value = edge_ref[side, f]
            value = pltpu.roll(value, turn, 1) if turn else value
            packed = jnp.where((lane >= at) & (lane < at + STEPS_AFTER), value, packed)
    seen_ref[:, index_ref.shape[0]:] = packed


def inverse(matrix, low):
    size = matrix.shape[0]
    row = lax.broadcasted_iota(jnp.int32, (size, size), 0)
    eye = (row == lax.broadcasted_iota(jnp.int32, (size, size), 1)).astype(jnp.float32)
    high = jnp.max(jnp.sum(jnp.abs(matrix), axis=1))
    delta = (high - low) / (high + low)

    def more(carry):
        return carry[0] > 1e-7

    def turn(carry):
        delta, guess = carry
        square = delta * delta
        scale = 2.0 / (2.0 - square)
        residual = 2.0 * eye - product(matrix, guess, ((1,), (0,)))
        return square / (2.0 - square), scale * product(guess, residual, ((1,), (0,)))

    return lax.while_loop(more, turn, (delta, eye * (2.0 / (high + low))))[1]


def gain_kernel(me_ref, seen_ref, value_ref, variance_ref, perturb_ref, weights_ref, edge_ref, *, parts):
    count = seen_ref.shape[0]
    members = count // parts
    observed = value_ref.shape[1]
    me = me_ref[0]

    def rows_of(ref, sign):
        pieces = []
        for away in range(parts):
            part = lax.rem(me + sign * away + parts, parts)
            pieces.append(ref[pl.ds(pl.multiple_of(part * members, members), members), :])
        return jnp.concatenate(pieces, axis=0)

    from_rows = rows_of(seen_ref, -1)
    to_rows = rows_of(seen_ref, 1)[:, :observed]
    predicted = from_rows[:, :observed]
    spread = predicted - jnp.sum(predicted, axis=0, keepdims=True) / count
    scaled = spread / variance_ref[...]
    innovation = value_ref[...] + rows_of(perturb_ref, 1) - to_rows
    row = lax.broadcasted_iota(jnp.int32, (count, count), 0)
    col = lax.broadcasted_iota(jnp.int32, (count, count), 1)
    inner = product(scaled, spread, ((1,), (1,))) + jnp.where(row == col, count - 1.0, 0.0)
    right = product(innovation, scaled, ((1,), (1,)))
    inverted = inverse(inner, count - 1.0)
    weights = product(right, inverted, ((1,), (0,)))
    weights = weights + product(right - product(weights, inner, ((1,), (0,))), inverted, ((1,), (0,)))
    to_member = lax.rem(me + row // members, parts) * members + row % members
    from_member = lax.rem(me - col // members + parts, parts) * members + col % members
    weights = weights + jnp.where(to_member == from_member, 1.0, 0.0)
    weights_ref[...] = weights
    edge_ref[...] = product(weights[:members], from_rows[:, observed:], ((1,), (0,)))


def apply_kernel(weights_ref, *refs):
    *block_refs, out_ref = refs
    parts, fields, members, block = out_ref.shape
    weights = weights_ref[...]
    for f in range(fields):
        stacked = jnp.concatenate([ref[f] for ref in block_refs], axis=0)
        out_ref[:, f] = product(weights, stacked, ((1,), (0,))).reshape(parts, members, block)


def place_kernel(me_ref, behind_ref, ahead_ref, *refs):
    *block_refs, out_ref, wide_ref, sems = refs
    parts = len(block_refs)
    fields, members, block = block_refs[0].shape
    columns = parts * block
    me = me_ref[0]
    for away in range(parts):
        start = pl.multiple_of(lax.rem(me - away + parts, parts) * block, LANES)
        for f in range(fields):
            wide_ref[f, :, pl.ds(start, block)] = block_refs[away][f]
    lane = lax.broadcasted_iota(jnp.int32, (members, LANES), 1)
    copies = []
    for f in range(fields):
        at = (fields + f) * STEPS_AFTER
        first = pltpu.roll(behind_ref[...], (LANES - at) % LANES, 1)
        wide_ref[f, :, :LANES] = wide_ref[f, :, :LANES] + jnp.where(lane < STEPS_AFTER, first, 0.0)
        at = f * STEPS_AFTER
        last = pltpu.roll(ahead_ref[...], (LANES - STEPS_AFTER - at) % LANES, 1)
        wide_ref[f, :, columns - LANES:] = wide_ref[f, :, columns - LANES:] + jnp.where(
            lane >= LANES - STEPS_AFTER, last, 0.0)
        copies.append(pltpu.make_async_copy(wide_ref.at[f], out_ref.at[f], sems.at[f]))
        copies[-1].start()
    for copy in copies:
        copy.wait()


def local(state, courant, angle, obs_index, obs_value, obs_variance, perturb):
    members, fields, columns = state.shape
    parts = lax.axis_size("mem")
    block = columns // parts
    observed = obs_index.shape[0]
    count = parts * members
    me = lax.axis_index("mem").astype(jnp.int32).reshape(1)
    float32 = functools.partial(jax.ShapeDtypeStruct, dtype=jnp.float32)

    coef = jnp.stack([courant, jnp.cos(angle), jnp.sin(angle)] + [courant] * (ROWS - 3))

    turned = state.transpose(1, 0, 2)

    def edge(lanes):
        own = state[:, :, lanes].transpose(1, 0, 2).reshape(fields * members, LANES)
        return jnp.concatenate([own, coef[:, lanes]], axis=0)

    behind = shifted(edge(slice(columns - LANES, columns)), "strip", 1)
    ahead = shifted(edge(slice(0, LANES)), "strip", -1)
    moved, seen = pl.pallas_call(
        advance_kernel,
        out_shape=(float32((parts, fields, members, block)), float32((members, observed + LANES))),
        in_specs=[SMEM, SMEM, ANY, VMEM, VMEM, VMEM],
        out_specs=(VMEM, VMEM),
        scratch_shapes=[
            pltpu.VMEM((fields, members, columns + 2 * LANES), jnp.float32),
            pltpu.VMEM((ROWS, columns + 2 * LANES), jnp.float32),
            pltpu.VMEM((members, columns), jnp.float32),
            pltpu.VMEM((2, fields, members, LANES), jnp.float32),
            pltpu.SemaphoreType.DMA((fields,)),
        ],
        name="advance",
    )(me, obs_index, turned, behind, ahead, coef)
    blocks = [moved[0]] + [shifted(moved[away], "mem", away) for away in range(1, parts)]
    all_seen = lax.all_gather(seen, "mem", axis=0, tiled=True)
    weights, edges = pl.pallas_call(
        functools.partial(gain_kernel, parts=parts),
        out_shape=(float32((count, count)), float32((members, LANES))),
        in_specs=[SMEM, VMEM, VMEM, VMEM, VMEM],
        out_specs=(VMEM, VMEM),
        name="gain",
    )(me, all_seen, obs_value.reshape(1, observed), obs_variance.reshape(1, observed), perturb)
    from_behind = shifted(edges, "strip", 1)
    from_ahead = shifted(edges, "strip", -1)
    mixed = pl.pallas_call(
        apply_kernel,
        out_shape=float32((parts, fields, members, block)),
        in_specs=[VMEM] * (1 + parts),
        out_specs=VMEM,
        name="mix",
    )(weights, *blocks)
    back = [mixed[0]] + [shifted(mixed[away], "mem", away) for away in range(1, parts)]
    placed = pl.pallas_call(
        place_kernel,
        out_shape=float32((fields, members, columns)),
        in_specs=[SMEM] + [VMEM] * (2 + parts),
        out_specs=ANY,
        scratch_shapes=[pltpu.VMEM((fields, members, columns), jnp.float32), pltpu.SemaphoreType.DMA((fields,))],
        name="place",
    )(me, from_behind, from_ahead, *back)
    return placed.transpose(1, 0, 2)


def solution(mesh):
    return jax.shard_map(
        local,
        mesh=mesh,
        in_specs=(
            P("mem", None, "strip"),
            P("strip"),
            P("strip"),
            P("strip"),
            P("strip"),
            P("strip"),
            P(None, "strip"),
        ),
        out_specs=P("mem", None, "strip"),
        check_vma=False,
    )
```

```python
import functools

import jax
import jax.numpy as jnp
from jax import lax
from jax.experimental import pallas as pl
from jax.experimental.pallas import tpu as pltpu
from jax.sharding import PartitionSpec as P

STEPS_BEFORE = 4
STEPS_AFTER = 2
LANES = 128
ROWS = 8

HIGH = lax.Precision.HIGHEST

VMEM = pl.BlockSpec(memory_space=pltpu.VMEM)
SMEM = pl.BlockSpec(memory_space=pltpu.SMEM)
ANY = pl.BlockSpec(memory_space=pl.ANY)


def limits(mebibytes):
    return pltpu.CompilerParams(vmem_limit_bytes=mebibytes << 20)


def shifted(block, axis, distance):
    count = lax.axis_size(axis)
    return lax.ppermute(block, axis, [(i, (i + distance) % count) for i in range(count)])


def swapped(block, axis, away):
    return lax.ppermute(block, axis, [(i, i ^ away) for i in range(lax.axis_size(axis))])


def trade_order(parts):
    return sorted(range(1, parts), key=lambda away: (away < 2, -bin(away >> 1).count("1"), away))


def product(left, right, contract):
    return lax.dot_general(left, right, (contract, ((), ())), precision=HIGH, preferred_element_type=jnp.float32)


def step(height, speed, across, courant, cosine, sine):
    width = height.shape[1]
    right_wave = speed + height
    left_wave = speed - height
    right_new = right_wave - courant * (right_wave - pltpu.roll(right_wave, 1, 1))
    left_new = left_wave + courant * (pltpu.roll(left_wave, width - 1, 1) - left_wave)
    speed_new = 0.5 * (right_new + left_new)
    height_new = 0.5 * (right_new - left_new)
    return height_new, cosine * speed_new + sine * across, cosine * across - sine * speed_new


def advance_kernel(me_ref, state_ref, coef_ref, out_ref, prior_ref):
    fields, members, columns = state_ref.shape
    parts, block = out_ref.shape[0], out_ref.shape[3]
    width = block + 2 * LANES
    me = me_ref[0]

    def one(away, _):
        start = pl.multiple_of((me ^ away) * block, LANES)
        left = pl.multiple_of(jnp.maximum(start - LANES, 0), LANES)
        right = pl.multiple_of(jnp.minimum(start + block, columns - LANES), LANES)

        def window(ref, *at):
            pieces = [ref[(*at, pl.ds(left, LANES))], ref[(*at, pl.ds(start, block))], ref[(*at, pl.ds(right, LANES))]]
            return jnp.concatenate(pieces, axis=1)

        coefs = [jnp.broadcast_to(window(coef_ref, slice(k, k + 1)), (ROWS, width)) for k in range(3)]
        for group in range(members // ROWS):
            rows = slice(group * ROWS, (group + 1) * ROWS)
            fields_now = [window(state_ref, f, rows) for f in range(fields)]
            for _ in range(STEPS_BEFORE):
                fields_now = step(*fields_now, *coefs)
            prior_ref[rows, pl.ds(start, block)] = fields_now[0][:, LANES:LANES + block]
            for _ in range(STEPS_AFTER):
                fields_now = step(*fields_now, *coefs)
            for f in range(fields):
                out_ref[away, f, rows, :] = fields_now[f][:, LANES:LANES + block]
        return 0

    lax.fori_loop(0, parts, one, 0)


REACH = STEPS_BEFORE + STEPS_AFTER
EACH = 2 * (REACH + STEPS_AFTER)


def lane_plan(field):
    base = field * EACH
    return {
        "first": (base, 0, REACH),
        "last": (base + REACH, LANES - REACH, REACH),
        "before": (base + 2 * REACH, LANES - STEPS_AFTER, STEPS_AFTER),
        "after": (base + 2 * REACH + STEPS_AFTER, 0, STEPS_AFTER),
    }


def edge_kernel(me_ref, tile_ref, turn_ref, first_ref, last_ref, behind_ref, ahead_ref, moved_ref, prior_ref, seen_ref,
                held_ref):
    parts, fields, members, block = moved_ref.shape
    columns = prior_ref.shape[1]
    observed = tile_ref.shape[0]
    me = me_ref[0]
    held_ref[...] = prior_ref[...]
    lane = lax.broadcasted_iota(jnp.int32, (members, LANES), 1)
    pieces = []
    for side, (left_ref, right_ref) in enumerate(((behind_ref, first_ref), (last_ref, ahead_ref))):
        both = jnp.concatenate([left_ref[...], right_ref[...]], axis=1)
        fields_now = [both[f * members:(f + 1) * members] for f in range(fields)]
        coefs = [both[fields * members + k:fields * members + k + 1] for k in range(3)]
        for _ in range(STEPS_BEFORE):
            fields_now = step(*fields_now, *coefs)
        inner = slice(LANES, 2 * LANES) if side == 0 else slice(0, LANES)
        height = fields_now[0][:, inner]
        if side == 0:
            held_ref[:, :LANES] = jnp.where(lane < REACH, height, held_ref[:, :LANES])
        else:
            held_ref[:, columns - LANES:] = jnp.where(lane >= LANES - REACH, height, held_ref[:, columns - LANES:])
        wide = lax.broadcasted_iota(jnp.int32, (members, 2 * LANES), 1)
        own = wide >= LANES if side == 0 else wide < LANES
        fields_now = [jnp.where(own, value, 0.0) for value in fields_now]
        for _ in range(STEPS_AFTER):
            fields_now = step(*fields_now, *coefs)
        pieces.append(fields_now)
    packed = jnp.zeros((members, LANES), jnp.float32)
    for f in range(fields):
        tiles = {
            "first": pieces[0][f][:, LANES:] - moved_ref[me, f, :, :LANES],
            "last": pieces[1][f][:, :LANES] - moved_ref[me ^ (parts - 1), f, :, block - LANES:],
            "before": pieces[0][f][:, :LANES],
            "after": pieces[1][f][:, LANES:],
        }
        for name, (put, cut, size) in lane_plan(f).items():
            turned = pltpu.roll(tiles[name], (put - cut) % LANES, 1) if put != cut else tiles[name]
            packed = jnp.where((lane >= put) & (lane < put + size), turned, packed)
    seen_ref[:, observed:] = packed

    for group in range(observed // LANES):
        def pick(o, held):
            at = group * LANES + o
            tile = held_ref[:, pl.ds(pl.multiple_of(tile_ref[at], LANES), LANES)]
            return jnp.where(lane == o, pltpu.roll(tile, turn_ref[at], 1), held)
        held = lax.fori_loop(0, LANES, pick, jnp.zeros((members, LANES), jnp.float32), unroll=16)
        seen_ref[:, group * LANES:(group + 1) * LANES] = held


def inverse(matrix, low):
    size = matrix.shape[0]
    row = lax.broadcasted_iota(jnp.int32, (size, size), 0)
    eye = (row == lax.broadcasted_iota(jnp.int32, (size, size), 1)).astype(jnp.float32)
    high = jnp.max(jnp.sum(jnp.abs(matrix), axis=1))
    delta = (high - low) / (high + low)

    def more(carry):
        return carry[0] > 1e-7

    def turn(carry):
        delta, guess = carry
        square = delta * delta
        scale = 2.0 / (2.0 - square)
        residual = 2.0 * eye - product(matrix, guess, ((1,), (0,)))
        return square / (2.0 - square), scale * product(guess, residual, ((1,), (0,)))

    return lax.while_loop(more, turn, (delta, eye * (2.0 / (high + low))))[1]


def gain_kernel(me_ref, value_ref, variance_ref, perturb_ref, *refs):
    *seen_refs, weights_ref, edge_ref = refs
    parts = len(seen_refs)
    members = seen_refs[0].shape[0]
    count = parts * members
    observed = value_ref.shape[1]
    me = me_ref[0]
    seen = jnp.concatenate([ref[...] for ref in seen_refs], axis=0)
    predicted = seen[:, :observed]
    perturb = jnp.concatenate(
        [perturb_ref[pl.ds(pl.multiple_of((me ^ away) * members, members), members), :] for away in range(parts)], axis=0)
    spread = predicted - jnp.sum(predicted, axis=0, keepdims=True) / count
    scaled = spread / variance_ref[...]
    innovation = value_ref[...] + perturb - predicted
    row = lax.broadcasted_iota(jnp.int32, (count, count), 0)
    col = lax.broadcasted_iota(jnp.int32, (count, count), 1)
    inner = product(scaled, spread, ((1,), (1,))) + jnp.where(row == col, count - 1.0, 0.0)
    right = product(innovation, scaled, ((1,), (1,)))
    inverted = inverse(inner, count - 1.0)
    weights = product(right, inverted, ((1,), (0,)))
    weights = weights + product(right - product(weights, inner, ((1,), (0,))), inverted, ((1,), (0,)))
    weights = weights + jnp.where(row == col, 1.0, 0.0)
    weights_ref[...] = weights
    edge_ref[...] = product(weights[:members], seen[:, observed:], ((1,), (0,)))


def apply_kernel(weights_ref, *refs):
    *block_refs, out_ref = refs
    parts, fields, members, block = out_ref.shape
    weights = weights_ref[...]
    for f in range(fields):
        stacked = jnp.concatenate([ref[f] for ref in block_refs], axis=0)
        out_ref[:, f] = product(weights, stacked, ((1,), (0,))).reshape(parts, members, block)


def place_kernel(me_ref, own_ref, behind_ref, ahead_ref, *refs):
    *block_refs, out_ref = refs
    parts = len(block_refs)
    fields, members, block = block_refs[0].shape
    columns = parts * block
    me = me_ref[0]
    for away in range(parts):
        start = pl.multiple_of((me ^ away) * block, LANES)
        for f in range(fields):
            out_ref[f, :, pl.ds(start, block)] = block_refs[away][f]
    lane = lax.broadcasted_iota(jnp.int32, (members, LANES), 1)

    def piece(ref, put, cut, size, to):
        value = pltpu.roll(ref[...], (to - put) % LANES, 1) if put != to else ref[...]
        return jnp.where((lane >= to) & (lane < to + size), value, 0.0)

    for f in range(fields):
        plan = lane_plan(f)
        first = piece(own_ref, *plan["first"], 0) + piece(behind_ref, *plan["after"], 0)
        last = piece(own_ref, *plan["last"], LANES - REACH) + piece(ahead_ref, *plan["before"], LANES - STEPS_AFTER)
        out_ref[f, :, :LANES] = out_ref[f, :, :LANES] + first
        out_ref[f, :, columns - LANES:] = out_ref[f, :, columns - LANES:] + last


def local(state, courant, angle, obs_index, obs_value, obs_variance, perturb):
    members, fields, columns = state.shape
    parts = lax.axis_size("mem")
    block = columns // parts
    observed = obs_index.shape[0]
    count = parts * members
    me = lax.axis_index("mem").astype(jnp.int32).reshape(1)
    float32 = functools.partial(jax.ShapeDtypeStruct, dtype=jnp.float32)

    coef = jnp.stack([courant, jnp.cos(angle), jnp.sin(angle)] + [courant] * (ROWS - 3))

    turned = state.transpose(1, 0, 2)

    def edge(lanes):
        own = state[:, :, lanes].transpose(1, 0, 2).reshape(fields * members, LANES)
        return jnp.concatenate([own, coef[:, lanes]], axis=0)

    order = trade_order(parts)

    def trade(blocks):
        traded = {away: swapped(blocks[away], "mem", away) for away in order}
        return [blocks[0]] + [traded[away] for away in range(1, parts)]

    tiles = obs_index & -LANES
    turns = (jnp.arange(observed, dtype=jnp.int32) - obs_index) & (LANES - 1)
    first, last = edge(slice(0, LANES)), edge(slice(columns - LANES, columns))
    behind = shifted(last, "strip", 1)
    ahead = shifted(first, "strip", -1)
    moved, prior = pl.pallas_call(
        advance_kernel,
        out_shape=(float32((parts, fields, members, block)), float32((members, columns))),
        in_specs=[SMEM, VMEM, VMEM],
        out_specs=(VMEM, VMEM),
        name="advance",
        compiler_params=limits(12),
    )(me, turned, coef)
    blocks = trade(moved)
    seen = pl.pallas_call(
        edge_kernel,
        out_shape=float32((members, observed + LANES)),
        in_specs=[SMEM] * 3 + [VMEM] * 6,
        out_specs=VMEM,
        scratch_shapes=[pltpu.VMEM((members, columns), jnp.float32)],
        name="observe",
        compiler_params=limits(12),
    )(me, tiles, turns, first, last, behind, ahead, moved, prior)
    weights, edges = pl.pallas_call(
        gain_kernel,
        out_shape=(float32((count, count)), float32((members, LANES))),
        in_specs=[SMEM] + [VMEM] * (3 + parts),
        out_specs=(VMEM, VMEM),
        name="gain",
        compiler_params=limits(12),
    )(me, obs_value.reshape(1, observed), obs_variance.reshape(1, observed), perturb, *trade([seen] * parts))
    from_behind = shifted(edges, "strip", 1)
    from_ahead = shifted(edges, "strip", -1)
    mixed = pl.pallas_call(
        apply_kernel,
        out_shape=float32((parts, fields, members, block)),
        in_specs=[VMEM] * (1 + parts),
        out_specs=VMEM,
        name="mix",
        compiler_params=limits(12),
    )(weights, *blocks)
    back = trade(mixed)
    placed = pl.pallas_call(
        place_kernel,
        out_shape=float32((fields, members, columns)),
        in_specs=[SMEM] + [VMEM] * (3 + parts),
        out_specs=VMEM,
        name="place",
        compiler_params=limits(12),
    )(me, edges, from_behind, from_ahead, *back)
    return placed.transpose(1, 0, 2)


def solution(mesh):
    return jax.shard_map(
        local,
        mesh=mesh,
        in_specs=(
            P("mem", None, "strip"),
            P("strip"),
            P("strip"),
            P("strip"),
            P("strip"),
            P("strip"),
            P(None, "strip"),
        ),
        out_specs=P("mem", None, "strip"),
        check_vma=False,
    )
```

```python
import functools

import jax
import jax.numpy as jnp
from jax import lax
from jax.experimental import pallas as pl
from jax.experimental.pallas import tpu as pltpu
from jax.sharding import PartitionSpec as P


STEPS_BEFORE = 4
STEPS_AFTER = 2
LANES = 128
ROWS = 8

HIGH = lax.Precision.HIGHEST

VMEM = pl.BlockSpec(memory_space=pltpu.VMEM)
SMEM = pl.BlockSpec(memory_space=pltpu.SMEM)
ANY = pl.BlockSpec(memory_space=pl.ANY)


def limits(mebibytes):
    return pltpu.CompilerParams(vmem_limit_bytes=mebibytes << 20)


def shifted(block, axis, distance):
    count = lax.axis_size(axis)
    return lax.ppermute(block, axis, [(i, (i + distance) % count) for i in range(count)])


def swapped(block, axis, away):
    return lax.ppermute(block, axis, [(i, i ^ away) for i in range(lax.axis_size(axis))])


def early_rounds(parts):
    return parts // 2


def trade_order(parts):
    return sorted(range(1, parts), key=lambda away: (away < 2, away % 2 if bin(away >> 1).count("1") == 1 else -1, away))


def product(left, right, contract):
    return lax.dot_general(left, right, (contract, ((), ())), precision=HIGH, preferred_element_type=jnp.float32)


def step(height, speed, across, courant, cosine, sine):
    width = height.shape[1]
    right_wave = speed + height
    left_wave = speed - height
    right_new = right_wave - courant * (right_wave - pltpu.roll(right_wave, 1, 1))
    left_new = left_wave + courant * (pltpu.roll(left_wave, width - 1, 1) - left_wave)
    speed_new = 0.5 * (right_new + left_new)
    height_new = 0.5 * (right_new - left_new)
    return height_new, cosine * speed_new + sine * across, cosine * across - sine * speed_new


def advance_kernel(me_ref, far_ref, far_courant_ref, far_angle_ref, out_ref, prior_ref, first_ref, last_ref,
                   state_ref, courant_ref, angle_ref, cosine_ref, sine_ref, sems, coef_sems):
    fields, members, columns = far_ref.shape
    parts, block = out_ref.shape[0], out_ref.shape[3]
    width = block + 2 * LANES
    me = me_ref[0]
    coef_refs = (courant_ref, cosine_ref, sine_ref)

    def fetch(part):
        lanes = pl.ds(pl.multiple_of(part * block, LANES), block)
        return pltpu.make_async_copy(far_ref.at[:, :, lanes], state_ref.at[:, :, lanes], sems.at[part])

    copies = [
        pltpu.make_async_copy(far_courant_ref, courant_ref, coef_sems.at[0]),
        pltpu.make_async_copy(far_angle_ref, angle_ref, coef_sems.at[1]),
    ]
    for copy in copies[::-1]:
        copy.start()
    for part in range(parts):
        fetch(part).start()
    for copy in copies:
        copy.wait()
    cosine_ref[...] = jnp.cos(angle_ref[...])
    sine_ref[...] = jnp.sin(angle_ref[...])
    fetch(0).wait()

    def one(part, _):
        @pl.when(part + 1 < parts)
        def _():
            fetch(part + 1).wait()

        away = me ^ part
        start = pl.multiple_of(part * block, LANES)
        left = pl.multiple_of(jnp.maximum(start - LANES, 0), LANES)
        right = pl.multiple_of(jnp.minimum(start + block, columns - LANES), LANES)

        def window(ref, *at):
            pieces = [ref[(*at, pl.ds(left, LANES))], ref[(*at, pl.ds(start, block))], ref[(*at, pl.ds(right, LANES))]]
            return jnp.concatenate(pieces, axis=1)

        coefs = [jnp.broadcast_to(window(ref, slice(0, 1)), (ROWS, width)) for ref in coef_refs]
        for group in range(members // ROWS):
            rows = slice(group * ROWS, (group + 1) * ROWS)
            fields_now = [window(state_ref, f, rows) for f in range(fields)]
            for _ in range(STEPS_BEFORE):
                fields_now = step(*fields_now, *coefs)
            for t in range(block // LANES):
                prior_ref[start // LANES + t, rows, :] = fields_now[0][:, (t + 1) * LANES:(t + 2) * LANES]
            for _ in range(STEPS_AFTER):
                fields_now = step(*fields_now, *coefs)
            for f in range(fields):
                out_ref[away, f, rows, :] = fields_now[f][:, LANES:LANES + block]
        return 0

    lax.fori_loop(0, parts, one, 0)
    for ref, lanes in ((first_ref, slice(0, LANES)), (last_ref, slice(columns - LANES, columns))):
        for f in range(fields):
            ref[f * members:(f + 1) * members, :] = state_ref[f, :, lanes]
        for k in range(ROWS):
            row = fields * members + k
            ref[row:row + 1, :] = coef_refs[min(k, 2)][:, lanes]


REACH = STEPS_BEFORE + STEPS_AFTER
EACH = 2 * (REACH + STEPS_AFTER)


def lane_plan(field):
    base = field * EACH
    return {
        "first": (base, 0, REACH),
        "last": (base + REACH, LANES - REACH, REACH),
        "before": (base + 2 * REACH, LANES - STEPS_AFTER, STEPS_AFTER),
        "after": (base + 2 * REACH + STEPS_AFTER, 0, STEPS_AFTER),
    }


def edge_kernel(me_ref, row_ref, mask_ref, first_ref, last_ref, behind_ref, ahead_ref, moved_ref, prior_ref, seen_ref,
                held_ref, turned_ref, picked_ref):
    parts, fields, members, block = moved_ref.shape
    tiles = prior_ref.shape[0]
    observed = row_ref.shape[0]
    me = me_ref[0]
    held_ref[...] = prior_ref[...]
    lane = lax.broadcasted_iota(jnp.int32, (members, LANES), 1)
    pieces = []
    for side, (left_ref, right_ref) in enumerate(((behind_ref, first_ref), (last_ref, ahead_ref))):
        both = jnp.concatenate([left_ref[...], right_ref[...]], axis=1)
        fields_now = [both[f * members:(f + 1) * members] for f in range(fields)]
        coefs = [both[fields * members + k:fields * members + k + 1] for k in range(3)]
        for _ in range(STEPS_BEFORE):
            fields_now = step(*fields_now, *coefs)
        inner = slice(LANES, 2 * LANES) if side == 0 else slice(0, LANES)
        height = fields_now[0][:, inner]
        if side == 0:
            held_ref[0] = jnp.where(lane < REACH, height, held_ref[0])
        else:
            held_ref[tiles - 1] = jnp.where(lane >= LANES - REACH, height, held_ref[tiles - 1])
        wide = lax.broadcasted_iota(jnp.int32, (members, 2 * LANES), 1)
        own = wide >= LANES if side == 0 else wide < LANES
        fields_now = [jnp.where(own, value, 0.0) for value in fields_now]
        for _ in range(STEPS_AFTER):
            fields_now = step(*fields_now, *coefs)
        pieces.append(fields_now)
    packed = jnp.zeros((members, LANES), jnp.float32)
    for f in range(fields):
        cuts = {
            "first": pieces[0][f][:, LANES:] - moved_ref[me, f, :, :LANES],
            "last": pieces[1][f][:, :LANES] - moved_ref[me ^ (parts - 1), f, :, block - LANES:],
            "before": pieces[0][f][:, :LANES],
            "after": pieces[1][f][:, LANES:],
        }
        for name, (put, cut, size) in lane_plan(f).items():
            turned = pltpu.roll(cuts[name], (put - cut) % LANES, 1) if put != cut else cuts[name]
            packed = jnp.where((lane >= put) & (lane < put + size), turned, packed)
    seen_ref[:, observed:] = packed

    group = LANES // members
    for q in range(tiles // group):
        block = held_ref[q * group:(q + 1) * group].reshape(LANES, LANES)
        turned_ref[q * LANES:(q + 1) * LANES, :] = block.T

    def pick(turn, _):
        for k in range(ROWS):
            o = turn * ROWS + k
            picked_ref[pl.ds(o, 1), :] = turned_ref[pl.ds(row_ref[o], 1), :]
        return 0

    lax.fori_loop(0, observed // ROWS, pick, 0, unroll=2)
    fold = lax.broadcasted_iota(jnp.int32, (members, LANES), 0) == lane % members
    kept = picked_ref[...] * mask_ref[...]
    seen_ref[:, :observed] = product(fold.astype(jnp.float32), kept, ((1,), (1,)))


def inverse(matrix, low):
    size = matrix.shape[0]
    row = lax.broadcasted_iota(jnp.int32, (size, size), 0)
    eye = (row == lax.broadcasted_iota(jnp.int32, (size, size), 1)).astype(jnp.float32)
    high = jnp.max(jnp.sum(jnp.abs(matrix), axis=0))
    delta = (high - low) / (high + low)

    def more(carry):
        return carry[0] > 2e-4

    def turn(carry):
        delta, guess = carry
        square = delta * delta
        scale = 2.0 / (2.0 - square)
        residual = 2.0 * eye - product(matrix, guess, ((1,), (0,)))
        return square / (2.0 - square), scale * product(guess, residual, ((1,), (0,)))

    return lax.while_loop(more, turn, (delta, eye * (2.0 / (high + low))))[1]


def gain_kernel(me_ref, value_ref, variance_ref, perturb_ref, *refs):
    *seen_refs, weights_ref, edge_ref = refs
    parts = len(seen_refs)
    members = seen_refs[0].shape[0]
    count = parts * members
    observed = value_ref.shape[1]
    me = me_ref[0]
    seen = jnp.concatenate([ref[...] for ref in seen_refs], axis=0)
    predicted = seen[:, :observed]
    perturb = jnp.concatenate(
        [perturb_ref[pl.ds(pl.multiple_of((me ^ away) * members, members), members), :] for away in range(parts)], axis=0)
    spread = predicted - jnp.sum(predicted, axis=0, keepdims=True) / count
    scaled = spread / variance_ref[...]
    innovation = value_ref[...] + perturb - predicted
    row = lax.broadcasted_iota(jnp.int32, (count, count), 0)
    col = lax.broadcasted_iota(jnp.int32, (count, count), 1)
    inner = product(scaled, spread, ((1,), (1,))) + jnp.where(row == col, count - 1.0, 0.0)
    right = product(innovation, scaled, ((1,), (1,)))
    inverted = inverse(inner, count - 1.0)
    weights = product(right, inverted, ((1,), (0,)))
    weights = weights + product(right - product(weights, inner, ((1,), (0,))), inverted, ((1,), (0,)))
    weights = weights + jnp.where(row == col, 1.0, 0.0)
    weights_ref[...] = weights
    edge_ref[...] = product(weights[:members], seen[:, observed:], ((1,), (0,)))


def apply_kernel(weights_ref, *refs):
    *block_refs, out_ref = refs
    parts, fields, members, block = out_ref.shape
    weights = weights_ref[...]
    for f in range(fields):
        stacked = jnp.concatenate([ref[f] for ref in block_refs], axis=0)
        out_ref[:, f] = product(weights, stacked, ((1,), (0,))).reshape(parts, members, block)


def place_kernel(me_ref, own_ref, behind_ref, ahead_ref, *refs):
    *block_refs, out_ref = refs
    parts = len(block_refs)
    fields, members, block = block_refs[0].shape
    columns = parts * block
    me = me_ref[0]
    for away in range(parts):
        start = pl.multiple_of((me ^ away) * block, LANES)
        for f in range(fields):
            out_ref[f, :, pl.ds(start, block)] = block_refs[away][f]
    lane = lax.broadcasted_iota(jnp.int32, (members, LANES), 1)

    def piece(ref, put, cut, size, to):
        value = pltpu.roll(ref[...], (to - put) % LANES, 1) if put != to else ref[...]
        return jnp.where((lane >= to) & (lane < to + size), value, 0.0)

    for f in range(fields):
        plan = lane_plan(f)
        first = piece(own_ref, *plan["first"], 0) + piece(behind_ref, *plan["after"], 0)
        last = piece(own_ref, *plan["last"], LANES - REACH) + piece(ahead_ref, *plan["before"], LANES - STEPS_AFTER)
        out_ref[f, :, :LANES] = out_ref[f, :, :LANES] + first
        out_ref[f, :, columns - LANES:] = out_ref[f, :, columns - LANES:] + last


def local(state, courant, angle, obs_index, obs_value, obs_variance, perturb):
    members, fields, columns = state.shape
    parts = lax.axis_size("mem")
    block = columns // parts
    observed = obs_index.shape[0]
    count = parts * members
    me = lax.axis_index("mem").astype(jnp.int32).reshape(1)
    float32 = functools.partial(jax.ShapeDtypeStruct, dtype=jnp.float32)

    turned = state.transpose(1, 0, 2)

    order = trade_order(parts)
    early = order[:early_rounds(parts)]

    def trade(blocks, order=order):
        traded = {}
        for away in order:
            traded[away] = swapped(blocks[away], "mem", away)
        return traded

    def row(vector):
        return vector.reshape(1, -1)

    group = LANES // members
    picks = obs_index // (LANES * group) * LANES + obs_index % LANES
    mask = (obs_index // LANES % group)[:, None] == jnp.arange(LANES, dtype=jnp.int32)[None, :] // members
    moved, prior, first, last = pl.pallas_call(
        advance_kernel,
        out_shape=(
            float32((parts, fields, members, block)),
            float32((columns // LANES, members, LANES)),
            float32((fields * members + ROWS, LANES)),
            float32((fields * members + ROWS, LANES)),
        ),
        in_specs=[SMEM] + [pl.BlockSpec(memory_space=pltpu.HBM)] * 3,
        out_specs=(VMEM,) * 4,
        scratch_shapes=[pltpu.VMEM((fields, members, columns), jnp.float32)]
        + [pltpu.VMEM((1, columns), jnp.float32)] * 4
        + [pltpu.SemaphoreType.DMA((parts,)), pltpu.SemaphoreType.DMA((2,))],
        name="advance",
        compiler_params=limits(12),
    )(me, *[pltpu.with_memory_space_constraint(array, pltpu.HBM) for array in (turned, row(courant), row(angle))])
    behind = shifted(last, "strip", 1)
    ahead = shifted(first, "strip", -1)
    traded = trade(moved, early)
    seen = pl.pallas_call(
        edge_kernel,
        out_shape=float32((members, observed + LANES)),
        in_specs=[SMEM] * 2 + [VMEM] * 7,
        out_specs=VMEM,
        scratch_shapes=[
            pltpu.VMEM((columns // LANES, members, LANES), jnp.float32),
            pltpu.VMEM((columns // group, LANES), jnp.float32),
            pltpu.VMEM((observed, LANES), jnp.float32),
        ],
        name="observe",
        compiler_params=limits(12),
    )(me, picks, mask.astype(jnp.float32), first, last, behind, ahead, moved, prior)
    all_seen = trade([seen] * parts)
    rest, seen = lax.optimization_barrier(([moved[away] for away in range(parts)], seen))
    traded.update(trade(rest, order[len(early):]))
    blocks = [moved[0]] + [traded[away] for away in range(1, parts)]
    weights, edges = pl.pallas_call(
        gain_kernel,
        out_shape=(float32((count, count)), float32((members, LANES))),
        in_specs=[SMEM] + [VMEM] * (3 + parts),
        out_specs=(VMEM, VMEM),
        name="gain",
        compiler_params=limits(12),
    )(me, obs_value.reshape(1, observed), obs_variance.reshape(1, observed), perturb, seen, *[all_seen[away] for away in range(1, parts)])
    from_behind = shifted(edges, "strip", 1)
    from_ahead = shifted(edges, "strip", -1)
    mixed = pl.pallas_call(
        apply_kernel,
        out_shape=float32((parts, fields, members, block)),
        in_specs=[VMEM] * (1 + parts),
        out_specs=VMEM,
        name="mix",
        compiler_params=limits(12),
    )(weights, *blocks)
    back = trade(mixed, sorted(order, key=lambda away: (away < 2, away % 2, away)))
    back = [mixed[0]] + [back[away] for away in range(1, parts)]
    placed = pl.pallas_call(
        place_kernel,
        out_shape=float32((fields, members, columns)),
        in_specs=[SMEM] + [VMEM] * (3 + parts),
        out_specs=VMEM,
        name="place",
        compiler_params=limits(12),
    )(me, edges, from_behind, from_ahead, *back)
    return placed.transpose(1, 0, 2)


def solution(mesh):
    return jax.shard_map(
        local,
        mesh=mesh,
        in_specs=(
            P("mem", None, "strip"),
            P("strip"),
            P("strip"),
            P("strip"),
            P("strip"),
            P("strip"),
            P(None, "strip"),
        ),
        out_specs=P("mem", None, "strip"),
        check_vma=False,
    )
```

```python
import functools

import jax
import jax.numpy as jnp
from jax import lax
from jax.experimental import pallas as pl
from jax.experimental.pallas import tpu as pltpu
from jax.sharding import PartitionSpec as P


STEPS_BEFORE = 4
STEPS_AFTER = 2
LANES = 128
ROWS = 8

HIGH = lax.Precision.HIGHEST

VMEM = pl.BlockSpec(memory_space=pltpu.VMEM)
SMEM = pl.BlockSpec(memory_space=pltpu.SMEM)
ANY = pl.BlockSpec(memory_space=pl.ANY)


def limits(mebibytes):
    return pltpu.CompilerParams(vmem_limit_bytes=mebibytes << 20)


def shifted(block, axis, distance):
    count = lax.axis_size(axis)
    return lax.ppermute(block, axis, [(i, (i + distance) % count) for i in range(count)])


def swapped(block, axis, away):
    return lax.ppermute(block, axis, [(i, i ^ away) for i in range(lax.axis_size(axis))])


def early_rounds(parts):
    return parts // 2


def trade_order(parts):
    return sorted(range(1, parts), key=lambda away: (away < 2, away % 2 if bin(away >> 1).count("1") == 1 else -1, away))


def back_order(parts):
    return sorted(range(1, parts), key=lambda away: (away < 2, away % 2, away))


def first_rounds(parts):
    return max(parts // 4, 1)


def product(left, right, contract):
    return lax.dot_general(left, right, (contract, ((), ())), precision=HIGH, preferred_element_type=jnp.float32)


def step(height, speed, across, courant, cosine, sine):
    width = height.shape[1]
    right_wave = speed + height
    left_wave = speed - height
    right_new = right_wave - courant * (right_wave - pltpu.roll(right_wave, 1, 1))
    left_new = left_wave + courant * (pltpu.roll(left_wave, width - 1, 1) - left_wave)
    speed_new = 0.5 * (right_new + left_new)
    height_new = 0.5 * (right_new - left_new)
    return height_new, cosine * speed_new + sine * across, cosine * across - sine * speed_new


def advance_kernel(me_ref, far_ref, far_courant_ref, far_angle_ref, out_ref, prior_ref, first_ref, last_ref,
                   state_ref, courant_ref, angle_ref, cosine_ref, sine_ref, sems, coef_sems):
    fields, members, columns = far_ref.shape
    parts, block = out_ref.shape[0], out_ref.shape[3]
    width = block + LANES
    me = me_ref[0]
    ahead_half = lax.broadcasted_iota(jnp.int32, (1, LANES), 1) < LANES // 2
    coef_refs = (courant_ref, cosine_ref, sine_ref)

    def fetch(part):
        lanes = pl.ds(pl.multiple_of(part * block, LANES), block)
        return pltpu.make_async_copy(far_ref.at[:, :, lanes], state_ref.at[:, :, lanes], sems.at[part])

    copies = [
        pltpu.make_async_copy(far_courant_ref, courant_ref, coef_sems.at[0]),
        pltpu.make_async_copy(far_angle_ref, angle_ref, coef_sems.at[1]),
    ]
    for copy in copies[::-1]:
        copy.start()
    for part in range(parts):
        fetch(part).start()
    for copy in copies:
        copy.wait()
    cosine_ref[...] = jnp.cos(angle_ref[...])
    sine_ref[...] = jnp.sin(angle_ref[...])
    fetch(0).wait()

    def one(part, _):
        @pl.when(part + 1 < parts)
        def _():
            fetch(part + 1).wait()

        away = me ^ part
        start = pl.multiple_of(part * block, LANES)
        left = pl.multiple_of(jnp.maximum(start - LANES, 0), LANES)
        right = pl.multiple_of(jnp.minimum(start + block, columns - LANES), LANES)

        def window(ref, *at):
            beside = jnp.where(ahead_half, ref[(*at, pl.ds(right, LANES))], ref[(*at, pl.ds(left, LANES))])
            return jnp.concatenate([ref[(*at, pl.ds(start, block))], beside], axis=1)

        coefs = [jnp.broadcast_to(window(ref, slice(0, 1)), (ROWS, width)) for ref in coef_refs]
        for group in range(members // ROWS):
            rows = slice(group * ROWS, (group + 1) * ROWS)
            fields_now = [window(state_ref, f, rows) for f in range(fields)]
            for _ in range(STEPS_BEFORE):
                fields_now = step(*fields_now, *coefs)
            for t in range(block // LANES):
                prior_ref[start // LANES + t, rows, :] = fields_now[0][:, t * LANES:(t + 1) * LANES]
            for _ in range(STEPS_AFTER):
                fields_now = step(*fields_now, *coefs)
            for f in range(fields):
                out_ref[away, f, rows, :] = fields_now[f][:, :block]
        return 0

    lax.fori_loop(0, parts, one, 0)
    for ref, lanes in ((first_ref, slice(0, LANES)), (last_ref, slice(columns - LANES, columns))):
        for f in range(fields):
            ref[f * members:(f + 1) * members, :] = state_ref[f, :, lanes]
        for k in range(ROWS):
            row = fields * members + k
            ref[row:row + 1, :] = coef_refs[min(k, 2)][:, lanes]


REACH = STEPS_BEFORE + STEPS_AFTER
EACH = 2 * (REACH + STEPS_AFTER)


def lane_plan(field):
    base = field * EACH
    return {
        "first": (base, 0, REACH),
        "last": (base + REACH, LANES - REACH, REACH),
        "before": (base + 2 * REACH, LANES - STEPS_AFTER, STEPS_AFTER),
        "after": (base + 2 * REACH + STEPS_AFTER, 0, STEPS_AFTER),
    }


def edge_kernel(me_ref, row_ref, mask_ref, first_ref, last_ref, behind_ref, ahead_ref, moved_ref, prior_ref, seen_ref,
                held_ref, turned_ref, picked_ref):
    parts, fields, members, block = moved_ref.shape
    tiles = prior_ref.shape[0]
    observed = row_ref.shape[0]
    me = me_ref[0]
    held_ref[...] = prior_ref[...]
    lane = lax.broadcasted_iota(jnp.int32, (members, LANES), 1)
    pieces = []
    for side, (left_ref, right_ref) in enumerate(((behind_ref, first_ref), (last_ref, ahead_ref))):
        both = jnp.concatenate([left_ref[...], right_ref[...]], axis=1)
        fields_now = [both[f * members:(f + 1) * members] for f in range(fields)]
        coefs = [both[fields * members + k:fields * members + k + 1] for k in range(3)]
        for _ in range(STEPS_BEFORE):
            fields_now = step(*fields_now, *coefs)
        inner = slice(LANES, 2 * LANES) if side == 0 else slice(0, LANES)
        height = fields_now[0][:, inner]
        if side == 0:
            held_ref[0] = jnp.where(lane < REACH, height, held_ref[0])
        else:
            held_ref[tiles - 1] = jnp.where(lane >= LANES - REACH, height, held_ref[tiles - 1])
        wide = lax.broadcasted_iota(jnp.int32, (members, 2 * LANES), 1)
        own = wide >= LANES if side == 0 else wide < LANES
        fields_now = [jnp.where(own, value, 0.0) for value in fields_now]
        for _ in range(STEPS_AFTER):
            fields_now = step(*fields_now, *coefs)
        pieces.append(fields_now)
    packed = jnp.zeros((members, LANES), jnp.float32)
    for f in range(fields):
        cuts = {
            "first": pieces[0][f][:, LANES:] - moved_ref[me, f, :, :LANES],
            "last": pieces[1][f][:, :LANES] - moved_ref[me ^ (parts - 1), f, :, block - LANES:],
            "before": pieces[0][f][:, :LANES],
            "after": pieces[1][f][:, LANES:],
        }
        for name, (put, cut, size) in lane_plan(f).items():
            turned = pltpu.roll(cuts[name], (put - cut) % LANES, 1) if put != cut else cuts[name]
            packed = jnp.where((lane >= put) & (lane < put + size), turned, packed)
    seen_ref[:, observed:] = packed

    group = LANES // members
    for q in range(tiles // group):
        block = held_ref[q * group:(q + 1) * group].reshape(LANES, LANES)
        turned_ref[q * LANES:(q + 1) * LANES, :] = block.T

    def pick(turn, _):
        for k in range(ROWS):
            o = turn * ROWS + k
            picked_ref[pl.ds(o, 1), :] = turned_ref[pl.ds(row_ref[o], 1), :]
        return 0

    lax.fori_loop(0, observed // ROWS, pick, 0, unroll=2)
    fold = lax.broadcasted_iota(jnp.int32, (members, LANES), 0) == lane % members
    kept = picked_ref[...] * mask_ref[...]
    seen_ref[:, :observed] = product(fold.astype(jnp.float32), kept, ((1,), (1,)))


def inverse(matrix, low):
    size = matrix.shape[0]
    row = lax.broadcasted_iota(jnp.int32, (size, size), 0)
    eye = (row == lax.broadcasted_iota(jnp.int32, (size, size), 1)).astype(jnp.float32)
    high = jnp.max(jnp.sum(jnp.abs(matrix), axis=0))
    delta = (high - low) / (high + low)

    def more(carry):
        return carry[0] > 2e-4

    def turn(carry):
        delta, guess = carry
        square = delta * delta
        scale = 2.0 / (2.0 - square)
        residual = 2.0 * eye - product(matrix, guess, ((1,), (0,)))
        return square / (2.0 - square), scale * product(guess, residual, ((1,), (0,)))

    return lax.while_loop(more, turn, (delta, eye * (2.0 / (high + low))))[1]


def gain_kernel(me_ref, value_ref, variance_ref, perturb_ref, *refs):
    *seen_refs, weights_ref, tail_ref = refs
    parts = len(seen_refs)
    members = seen_refs[0].shape[0]
    count = parts * members
    observed = value_ref.shape[1]
    me = me_ref[0]
    seen = jnp.concatenate([ref[...] for ref in seen_refs], axis=0)
    predicted = seen[:, :observed]
    perturb = jnp.concatenate(
        [perturb_ref[pl.ds(pl.multiple_of((me ^ away) * members, members), members), :] for away in range(parts)], axis=0)
    spread = predicted - jnp.sum(predicted, axis=0, keepdims=True) / count
    scaled = spread * (1.0 / variance_ref[...])
    innovation = value_ref[...] + perturb - predicted
    row = lax.broadcasted_iota(jnp.int32, (count, count), 0)
    col = lax.broadcasted_iota(jnp.int32, (count, count), 1)
    inner = product(scaled, spread, ((1,), (1,))) + jnp.where(row == col, count - 1.0, 0.0)
    right = product(innovation, scaled, ((1,), (1,)))
    inverted = inverse(inner, count - 1.0)
    weights = product(right, inverted, ((1,), (0,)))
    weights = weights + product(right - product(weights, inner, ((1,), (0,))), inverted, ((1,), (0,)))
    weights = weights + jnp.where(row == col, 1.0, 0.0)
    weights_ref[...] = weights
    tail_ref[...] = seen[:, observed:]


def apply_kernel(weights_ref, *refs, aways):
    *block_refs, out_ref = refs
    rounds, fields, members, block = out_ref.shape
    weights = jnp.concatenate([weights_ref[away * members:(away + 1) * members, :] for away in aways], axis=0)
    for f in range(fields):
        stacked = jnp.concatenate([ref[f] for ref in block_refs], axis=0)
        out_ref[:, f] = product(weights, stacked, ((1,), (0,))).reshape(rounds, members, block)


def tail_kernel(weights_ref, tail_ref, edge_ref):
    edge_ref[...] = product(weights_ref[:edge_ref.shape[0], :], tail_ref[...], ((1,), (0,)))


def place_kernel(me_ref, own_ref, behind_ref, ahead_ref, *refs):
    *block_refs, out_ref = refs
    parts = len(block_refs)
    fields, members, block = block_refs[0].shape
    columns = parts * block
    me = me_ref[0]
    for away in range(parts):
        start = pl.multiple_of((me ^ away) * block, LANES)
        for f in range(fields):
            out_ref[f, :, pl.ds(start, block)] = block_refs[away][f]
    lane = lax.broadcasted_iota(jnp.int32, (members, LANES), 1)

    def piece(ref, put, cut, size, to):
        value = pltpu.roll(ref[...], (to - put) % LANES, 1) if put != to else ref[...]
        return jnp.where((lane >= to) & (lane < to + size), value, 0.0)

    for f in range(fields):
        plan = lane_plan(f)
        first = piece(own_ref, *plan["first"], 0) + piece(behind_ref, *plan["after"], 0)
        last = piece(own_ref, *plan["last"], LANES - REACH) + piece(ahead_ref, *plan["before"], LANES - STEPS_AFTER)
        out_ref[f, :, :LANES] = out_ref[f, :, :LANES] + first
        out_ref[f, :, columns - LANES:] = out_ref[f, :, columns - LANES:] + last


def local(state, courant, angle, obs_index, obs_value, obs_variance, perturb):
    members, fields, columns = state.shape
    parts = lax.axis_size("mem")
    block = columns // parts
    observed = obs_index.shape[0]
    count = parts * members
    me = lax.axis_index("mem").astype(jnp.int32).reshape(1)
    float32 = functools.partial(jax.ShapeDtypeStruct, dtype=jnp.float32)

    turned = state.transpose(1, 0, 2)

    order = trade_order(parts)
    early = order[:early_rounds(parts)]

    def trade(blocks, order=order):
        traded = {}
        for away in order:
            traded[away] = swapped(blocks[away], "mem", away)
        return traded

    def row(vector):
        return vector.reshape(1, -1)

    group = LANES // members
    picks = obs_index // (LANES * group) * LANES + obs_index % LANES
    mask = (obs_index // LANES % group)[:, None] == jnp.arange(LANES, dtype=jnp.int32)[None, :] // members
    moved, prior, first, last = pl.pallas_call(
        advance_kernel,
        out_shape=(
            float32((parts, fields, members, block)),
            float32((columns // LANES, members, LANES)),
            float32((fields * members + ROWS, LANES)),
            float32((fields * members + ROWS, LANES)),
        ),
        in_specs=[SMEM] + [pl.BlockSpec(memory_space=pltpu.HBM)] * 3,
        out_specs=(VMEM,) * 4,
        scratch_shapes=[pltpu.VMEM((fields, members, columns), jnp.float32)]
        + [pltpu.VMEM((1, columns), jnp.float32)] * 4
        + [pltpu.SemaphoreType.DMA((parts,)), pltpu.SemaphoreType.DMA((2,))],
        name="advance",
        compiler_params=limits(12),
    )(me, *[pltpu.with_memory_space_constraint(array, pltpu.HBM) for array in (turned, row(courant), row(angle))])
    behind = shifted(last, "strip", 1)
    ahead = shifted(first, "strip", -1)
    traded = trade(moved, early)
    seen = pl.pallas_call(
        edge_kernel,
        out_shape=float32((members, observed + LANES)),
        in_specs=[SMEM] * 2 + [VMEM] * 7,
        out_specs=VMEM,
        scratch_shapes=[
            pltpu.VMEM((columns // LANES, members, LANES), jnp.float32),
            pltpu.VMEM((columns // group, LANES), jnp.float32),
            pltpu.VMEM((observed, LANES), jnp.float32),
        ],
        name="observe",
        compiler_params=limits(12),
    )(me, picks, mask.astype(jnp.float32), first, last, behind, ahead, moved, prior)
    all_seen = trade([seen] * parts)
    rest, seen = lax.optimization_barrier(([moved[away] for away in range(parts)], seen))
    traded.update(trade(rest, order[len(early):]))
    blocks = [moved[0]] + [traded[away] for away in range(1, parts)]
    weights, tail = pl.pallas_call(
        gain_kernel,
        out_shape=(float32((count, count)), float32((count, LANES))),
        in_specs=[SMEM] + [VMEM] * (3 + parts),
        out_specs=(VMEM, VMEM),
        name="gain",
        compiler_params=limits(12),
    )(me, obs_value.reshape(1, observed), obs_variance.reshape(1, observed), perturb, seen, *[all_seen[away] for away in range(1, parts)])

    def mix(aways):
        mixed = pl.pallas_call(
            functools.partial(apply_kernel, aways=aways),
            out_shape=float32((len(aways), fields, members, block)),
            in_specs=[VMEM] * (1 + parts),
            out_specs=VMEM,
            name="mix",
            compiler_params=limits(12),
        )(weights, *blocks)
        return {away: mixed[turn] for turn, away in enumerate(aways)}

    order = back_order(parts)
    ahead_count = first_rounds(parts)
    mixed = mix(order[:ahead_count])
    mixed.update(mix(order[ahead_count:] + [0]))
    back = {0: mixed[0], **trade(mixed, order)}
    edges = pl.pallas_call(
        tail_kernel,
        out_shape=float32((members, LANES)),
        in_specs=[VMEM] * 2,
        out_specs=VMEM,
        name="tail",
        compiler_params=limits(12),
    )(weights, tail)
    from_behind = shifted(edges, "strip", 1)
    from_ahead = shifted(edges, "strip", -1)
    placed = pl.pallas_call(
        place_kernel,
        out_shape=float32((fields, members, columns)),
        in_specs=[SMEM] + [VMEM] * (3 + parts),
        out_specs=VMEM,
        name="place",
        compiler_params=limits(12),
    )(me, edges, from_behind, from_ahead, *[back[away] for away in range(parts)])
    return placed.transpose(1, 0, 2)


def solution(mesh):
    return jax.shard_map(
        local,
        mesh=mesh,
        in_specs=(
            P("mem", None, "strip"),
            P("strip"),
            P("strip"),
            P("strip"),
            P("strip"),
            P("strip"),
            P(None, "strip"),
        ),
        out_specs=P("mem", None, "strip"),
        check_vma=False,
    )
```
